32 devices in a mesh: row: 4 (over y, x), col: 8 (over z, core).
Axes of the slice: x: 2, y: 2, z: 4, core: 2. Of those that a mesh axis runs over, the one named last changes fastest.
Arguments:
- x_iterate: float32 [2048, 2048], P('row', 'col'), may hold values from -6 to 6
- z_inverse: float32 [2048, 2048], P('row', 'col'), may hold values from -0.25 to 0.25
- edge_src: int32 [8, 8, 64], P('row', 'col'), may hold values from 0 to 255
- edge_dst: int32 [8, 8, 64], P('row', 'col'), may hold values from 0 to 255
- edge_count: int32 [8, 8], P('row', 'col'), may hold values from 1 to 64, as said below
Outputs:
- schur_row: float32 [8, 8, 64], P('row', 'col')
The draws below stay inside these ranges and needn't reach their ends.
Inputs may be any that keep to these rules, and one draw needn't show every extreme that they name: `edge_count`: slots at and beyond a block pair's count are ignored; some block pair has all 64 slots live in every draw.
All inputs are finite; a program needn't handle non-finite values.
Results may differ from the reference program's by a relative error of at most 0.0001.
Values sent between devices are 32-bit elements; how exact they have to be, the bound alone decides.
No kernel may reach another device: no remote copies, remote signals or barrier semaphores. Data moves between devices by JAX's collectives and lax.ppermute only.
A program may use at most 64 MiB of HBM per device.

```python
import jax
import jax.numpy as jnp
from jax import lax

BLOCK = 256
CAP = 64
STEPS = 2
GRID = 8
ORDER = 2048


def draw_edge_count(key, part):
    key_one = jax.random.fold_in(key, 11)
    key_two = jax.random.fold_in(key, 23)
    key_three = jax.random.fold_in(key, 37)
    first = jax.random.randint(key_one, (GRID, GRID), 0, CAP)
    second = jax.random.randint(key_two, (GRID, GRID), 0, CAP)
    counts = CAP - first * second // (2 * CAP)
    chosen = jax.random.randint(key_three, (), 0, GRID * GRID)
    counts = counts.reshape(-1).at[chosen].set(CAP)
    return counts.reshape(GRID, GRID).astype(jnp.int32)


def with_ends(drawn, stream_key, least, largest):
    longest = drawn.shape.index(max(drawn.shape))
    spots = []
    for shift in (0, 1):
        where = [jax.random.randint(jax.random.fold_in(stream_key, axis), (), 0, length) for axis, length in enumerate(drawn.shape)]
        where[longest] = (where[longest] + shift) % drawn.shape[longest]
        spots.append(tuple(where))
    return drawn.at[spots[0]].set(least).at[spots[1]].set(largest)


def level_of(stream_key, shape, pieces, smallest, top_value):
    level = 1.0
    for dim, parts in pieces:
        heights = jax.random.uniform(jax.random.fold_in(jax.random.fold_in(stream_key, 6), dim), (parts,), jnp.float32, smallest / len(pieces), top_value / len(pieces))
        level = level * jnp.repeat(jnp.exp(heights), shape[dim] // parts).reshape((-1,) + (1,) * (len(shape) - 1 - dim))
    return level


def scatter_about(own_key, shape, spread, reach, pieces=(), kind=jnp.bfloat16):
    entries = jax.random.normal(own_key, shape, jnp.float32) * spread
    if len(pieces) > 0:
        entries = level_of(own_key, shape, pieces, -0.22, 0.18) * entries
    return jnp.clip(entries, min=-reach, max=reach).astype(kind)


def setup_inputs(seed: int = 0) -> dict:
    keys = jax.random.split(jax.random.key(seed), 6)
    x_iterate = scatter_about(keys[0], (ORDER, ORDER), 1.0, 6.0, ((0, 4), (1, 8)), jnp.float32)
    z_inverse = scatter_about(keys[1], (ORDER, ORDER), (2 * BLOCK) ** -0.5, 0.25, ((0, 4), (1, 8)), jnp.float32)
    edge_src = with_ends(jax.random.randint(keys[2], (GRID, GRID, CAP), 0, BLOCK), jax.random.fold_in(keys[2], 1), 0, BLOCK - 1).astype(jnp.int32)
    edge_dst = with_ends(jax.random.randint(keys[3], (GRID, GRID, CAP), 0, BLOCK), jax.random.fold_in(keys[3], 1), 0, BLOCK - 1).astype(jnp.int32)
    edge_count = draw_edge_count(jax.random.fold_in(keys[5], 71), 0)
    return {"x_iterate": x_iterate, "z_inverse": z_inverse, "edge_src": edge_src, "edge_dst": edge_dst, "edge_count": edge_count}


def reference(x_iterate, z_inverse, edge_src, edge_dst, edge_count):
    x_blocks = x_iterate.reshape(GRID, BLOCK, GRID, BLOCK).transpose(0, 2, 1, 3)
    z_blocks = z_inverse.reshape(GRID, BLOCK, GRID, BLOCK).transpose(0, 2, 1, 3)
    first = jnp.arange(GRID, dtype=jnp.int32)[:, None]
    second = jnp.arange(GRID, dtype=jnp.int32)[None, :]
    product = jnp.zeros((GRID, GRID, BLOCK, BLOCK), jnp.float32)
    for step in range(STEPS):
        inner = ((first + second + step) % GRID).astype(jnp.int32)
        left = x_blocks[first, inner]
        right = z_blocks[inner, second]
        product = product + jnp.einsum("ijab,ijbc->ijac", left, right, precision=lax.Precision.HIGHEST)
    flat = product.reshape(GRID, GRID, BLOCK * BLOCK)
    index = (edge_src * BLOCK + edge_dst).astype(jnp.int32)
    values = jnp.take_along_axis(flat, index, axis=2)
    live = jnp.arange(CAP, dtype=jnp.int32)[None, None, :] < edge_count[:, :, None]
    return jnp.where(live, values, jnp.zeros_like(values))
```

```python
import functools

import jax
import jax.numpy as jnp
from jax import lax
from jax.experimental import pallas as pl
from jax.experimental.pallas import tpu as pltpu
from jax.sharding import PartitionSpec as P

AXES = ("row", "col")


def send(shard, dest):
    n_row, n_col = lax.axis_size("row"), lax.axis_size("col")
    pairs = []
    for r in range(n_row):
        for c in range(n_col):
            to_r, to_c = dest(r, c)
            pairs.append((r * n_col + c, to_r % n_row * n_col + to_c % n_col))
    return lax.ppermute(shard, AXES, pairs)


def pieces(value):
    high = value.astype(jnp.bfloat16)
    rest = value - high.astype(jnp.float32)
    middle = rest.astype(jnp.bfloat16)
    low = (rest - middle.astype(jnp.float32)).astype(jnp.bfloat16)
    return high, middle, low


def pick(index, width):
    slots = index.shape[1]
    on_diagonal = lax.broadcasted_iota(jnp.int32, (slots, slots), 0) == lax.broadcasted_iota(jnp.int32, (slots, slots), 1)
    column = jnp.sum(jnp.where(on_diagonal, jnp.broadcast_to(index, (slots, slots)), 0), axis=1, keepdims=True)
    return column == lax.broadcasted_iota(jnp.int32, (slots, width), 1)


def gather_rows_kernel(cells, width, *refs):
    index_refs, x_ref, out_refs = refs[: cells + 1], refs[cells + 1], refs[cells + 2 :]
    slots = index_refs[0].shape[2]
    for cell in range(cells):
        chosen = jnp.concatenate(
            [pick(index_refs[cell + step][cell], width) for step in range(2)], axis=0
        ).astype(jnp.float32).astype(jnp.bfloat16)
        block = x_ref[cell * width : (cell + 1) * width, :]
        rows = sum(
            jnp.dot(chosen, piece, preferred_element_type=jnp.float32) for piece in pieces(block)
        )
        out_refs[cell][0:slots, :] = rows[:slots]
        at = out_refs[cell + 1].shape[0] - slots
        out_refs[cell + 1][at:, :] = rows[slots:]


def finish_kernel(cells, width, *refs):
    x_refs = refs[: cells + 1]
    whole_ref, part_ref, dst_ref, count_ref, out_ref = refs[cells + 1 :]
    part = part_ref.shape[0]
    first = lax.axis_index("col") % cells
    late = (first * 2 + 1 >= cells).astype(jnp.int32)
    slots = dst_ref.shape[2]
    totals = [jnp.zeros((slots, width), jnp.float32) for _ in range(cells)]
    for shift in range(cells + 1):
        held = [cell for cell in (shift, shift - 1) if 0 <= cell < cells]
        at = first + shift
        wrapped = (at >= cells).astype(jnp.int32)
        at = at - cells * wrapped
        at_part = jnp.clip(at - late * (cells - part), 0, part - 1)
        block = jnp.where(wrapped == late, whole_ref[at], part_ref[at_part])
        chosen = jnp.concatenate([pick(dst_ref[cell], width) for cell in held], axis=0).astype(jnp.float32).astype(jnp.bfloat16)
        columns = sum(
            lax.dot_general(chosen, piece, (((1,), (1,)), ((), ())), preferred_element_type=jnp.float32)
            for piece in pieces(block)
        )
        terms = columns * x_refs[shift][...]
        for place, cell in enumerate(held):
            totals[cell] = totals[cell] + terms[place * slots : (place + 1) * slots]
    on_diagonal = lax.broadcasted_iota(jnp.int32, (slots, slots), 0) == lax.broadcasted_iota(jnp.int32, (slots, slots), 1)
    slot = lax.broadcasted_iota(jnp.int32, (1, slots), 1)
    for cell in range(cells):
        values = jnp.sum(totals[cell], axis=1, keepdims=True)
        line = jnp.sum(jnp.where(on_diagonal, jnp.broadcast_to(values, (slots, slots)), 0.0), axis=0, keepdims=True)
        out_ref[cell] = jnp.where(slot < count_ref[cell], line, 0.0)


def body(x_iterate, z_inverse, edge_src, edge_dst, edge_count):
    width = x_iterate.shape[1]
    cells = x_iterate.shape[0] // width
    slots = edge_src.shape[2]
    vmem = pl.BlockSpec(memory_space=pltpu.VMEM)
    z_cells = z_inverse.reshape(cells, width, width)
    indices = [send(edge_src, lambda r, c, d=d: (r, c + cells * r + d)) for d in range(cells + 1)]
    part = (cells + 1) // 2
    late = lax.axis_index("col") % cells * 2 + 1 >= cells
    z_some = jnp.where(late, z_cells[cells - part :], z_cells[:part])

    def beyond(c):
        return (c % cells * 2 + 1 >= cells) * 1

    z_whole = send(z_inverse, lambda r, c: (r - c // cells - beyond(c), c))
    z_part = send(z_some, lambda r, c: (r - c // cells - 1 + beyond(c), c))
    sizes = [slots * sum(0 <= cell < cells for cell in (d, d - 1)) for d in range(cells + 1)]
    rows = pl.pallas_call(
        functools.partial(gather_rows_kernel, cells, width),
        out_shape=[jax.ShapeDtypeStruct((size, width), jnp.float32) for size in sizes],
        in_specs=[vmem] * (cells + 2),
        out_specs=[vmem] * (cells + 1),
        compiler_params=pltpu.CompilerParams(vmem_limit_bytes=8 * 2**20),
        name="gather_rows",
    )(*indices, x_iterate)
    x_moved = [send(rows[d], lambda r, c, d=d: (r, c - cells * r - d)) for d in range(cells + 1)]
    return pl.pallas_call(
        functools.partial(finish_kernel, cells, width),
        out_shape=jax.ShapeDtypeStruct((cells, 1, slots), jnp.float32),
        in_specs=[vmem] * (cells + 5),
        out_specs=vmem,
        compiler_params=pltpu.CompilerParams(vmem_limit_bytes=8 * 2**20),
        name="finish",
    )(*x_moved, z_whole.reshape(z_cells.shape), z_part, edge_dst, edge_count.reshape(cells, 1, 1))


def solution(mesh):
    return jax.shard_map(
        body,
        mesh=mesh,
        in_specs=(
            P("row", "col"),
            P("row", "col"),
            P("row", "col", None),
            P("row", "col", None),
            P("row", "col"),
        ),
        out_specs=P("row", "col", None),
        check_vma=False,
    )
```

```python
import functools

import jax
import jax.numpy as jnp
from jax import lax
from jax.experimental import pallas as pl
from jax.experimental.pallas import tpu as pltpu
from jax.sharding import PartitionSpec as P


AXES = ("row", "col")
VMEM = pl.BlockSpec(memory_space=pltpu.VMEM)
PARAMS = pltpu.CompilerParams(vmem_limit_bytes=8 * 2**20)

TERMS = tuple(
    tuple((a, b, s) for a in range(2) for b in range(2) for s in range(2) if (a + b + s) // 2 == side)
    for side in range(2)
)


def send(shard, dest):
    n_row, n_col = lax.axis_size("row"), lax.axis_size("col")
    pairs = []
    for r in range(n_row):
        for c in range(n_col):
            to_r, to_pair, to_side = dest(r, c // 2, c % 2)
            to_c = to_pair * 2 + to_side
            pairs.append((r * n_col + c, to_r % n_row * n_col + to_c % n_col))
    return lax.ppermute(shard, AXES, pairs)


def swap(shard):
    return send(shard, lambda r, pair, side: (r, pair, 1 - side))


def pieces(value):
    high = value.astype(jnp.bfloat16)
    rest = value - high.astype(jnp.float32)
    middle = rest.astype(jnp.bfloat16)
    low = (rest - middle.astype(jnp.float32)).astype(jnp.bfloat16)
    return high, middle, low


def diagonal(slots):
    return lax.broadcasted_iota(jnp.int32, (slots, slots), 0) == lax.broadcasted_iota(jnp.int32, (slots, slots), 1)


def pick(lines, width):
    columns = []
    for line in lines:
        slots = line.shape[1]
        spread = jnp.where(diagonal(slots), jnp.broadcast_to(line, (slots, slots)), 0)
        columns.append(jnp.sum(spread, axis=1, keepdims=True))
    column = jnp.concatenate(columns, axis=0)
    chosen = column == lax.broadcasted_iota(jnp.int32, (column.shape[0], width), 1)
    return chosen.astype(jnp.float32).astype(jnp.bfloat16)


def by_side(action):
    here = lax.axis_index("col") % 2
    for side in range(2):
        pl.when(here == side)(functools.partial(action, side))


def gather(side, block_of, index_ref, refs, out_ref, contract):
    slots = index_ref.shape[2]
    blocks = {}
    for place, (a, b, s) in enumerate(TERMS[side]):
        blocks.setdefault(block_of(a, b, a + b + s - 2 * side), []).append((place, a, b))
    for (which, at), wanted in blocks.items():
        width = out_ref.shape[1]
        chosen = pick([index_ref[(b ^ side) * 2 + a] for _, a, b in wanted], width)
        block = refs[which][at * width : (at + 1) * width, :]
        taken = sum(
            lax.dot_general(chosen, piece, (((1,), (contract,)), ((), ())), preferred_element_type=jnp.float32)
            for piece in pieces(block)
        )
        for n, (place, _, _) in enumerate(wanted):
            out_ref[place * slots : (place + 1) * slots, :] = taken[n * slots : (n + 1) * slots]


def gather_x_kernel(index_ref, own_ref, partner_ref, out_ref):
    @by_side
    def _(side):
        gather(side, lambda a, b, g: (g ^ side, a), index_ref, (own_ref, partner_ref), out_ref, 0)


def gather_z_kernel(index_ref, own_ref, partner_ref, out_ref):
    @by_side
    def _(side):
        def block_of(a, b, g):
            return (0, g) if b == side else (1, 0)

        gather(side, block_of, index_ref, (own_ref, partner_ref), out_ref, 1)


def dots_kernel(x_ref, z_ref, own_ref, other_ref):
    slots = own_ref.shape[2]

    def line(values):
        spread = jnp.where(diagonal(slots), jnp.broadcast_to(values, (slots, slots)), 0.0)
        return jnp.sum(spread, axis=0, keepdims=True)

    @by_side
    def _(side):
        products = [x_ref[n * slots : (n + 1) * slots, :] * z_ref[n * slots : (n + 1) * slots, :] for n in range(len(TERMS[side]))]
        for b in range(2):
            for a in range(2):
                mine = [products[n] for n, term in enumerate(TERMS[side]) if term[:2] == (a, b)]
                if mine:
                    out = line(jnp.sum(sum(mine[1:], mine[0]), axis=1, keepdims=True))
                    if b == side:
                        own_ref[a] = out
                    else:
                        other_ref[0] = out


def finish_kernel(own_ref, other_ref, count_ref, out_ref):
    slots = out_ref.shape[2]
    slot = lax.broadcasted_iota(jnp.int32, (1, slots), 1)
    shared = 1 - lax.axis_index("col") % 2
    for a in range(2):
        value = own_ref[a] + jnp.where(shared == a, other_ref[0], 0.0)
        out_ref[a] = jnp.where(slot < count_ref[a], value, 0.0)


def call(kernel, shapes, *operands):
    return pl.pallas_call(
        kernel,
        out_shape=[jax.ShapeDtypeStruct(shape, jnp.float32) for shape in shapes],
        in_specs=[VMEM] * len(operands),
        out_specs=[VMEM] * len(shapes),
        compiler_params=PARAMS,
    )(*operands)


def body(x_iterate, z_inverse, edge_src, edge_dst, edge_count):
    width = x_iterate.shape[1]
    slots = edge_src.shape[2]
    assert x_iterate.shape[0] == 2 * width
    side = lax.axis_index("col") % 2
    src_partner = swap(edge_src)
    dst_partner = swap(edge_dst)
    x_partner = swap(x_iterate)
    z_partner = swap(lax.dynamic_slice_in_dim(z_inverse, side * width, width, axis=0))
    src = jnp.concatenate([edge_src, src_partner], axis=0)
    dst = jnp.concatenate([edge_dst, dst_partner], axis=0)
    src = send(src, lambda r, pair, side: (r, pair + r + side, side))
    dst = send(dst, lambda r, pair, side: (r + pair + side, pair, side))
    terms = [(len(TERMS[0]) * slots, width)]
    (rows,) = call(gather_x_kernel, terms, src, x_iterate, x_partner)
    rows = send(rows, lambda r, pair, side: (r, pair - r - side, side))
    (columns,) = call(gather_z_kernel, terms, dst, z_inverse, z_partner)
    columns = send(columns, lambda r, pair, side: (r - pair - side, pair, side))
    own, other = call(dots_kernel, [(2, 1, slots), (1, 1, slots)], rows, columns)
    other = swap(other)
    (out,) = call(finish_kernel, [(2, 1, slots)], own, other, edge_count.reshape(2, 1, 1))
    return out


def solution(mesh):
    return jax.shard_map(
        body,
        mesh=mesh,
        in_specs=(
            P("row", "col"),
            P("row", "col"),
            P("row", "col", None),
            P("row", "col", None),
            P("row", "col"),
        ),
        out_specs=P("row", "col", None),
        check_vma=False,
    )
```

```python
import functools

import jax
import jax.numpy as jnp
from jax import lax
from jax.experimental import pallas as pl
from jax.experimental.pallas import tpu as pltpu
from jax.sharding import PartitionSpec as P


AXES = ("row", "col")
VMEM = pl.BlockSpec(memory_space=pltpu.VMEM)
PARAMS = pltpu.CompilerParams(vmem_limit_bytes=8 * 2**20)

TERMS = tuple(
    tuple((a, b, s) for a in range(2) for b in range(2) for s in range(2) if (a + b + s) // 2 == side)
    for side in range(2)
)


def send(shard, dest):
    n_row, n_col = lax.axis_size("row"), lax.axis_size("col")
    pairs = []
    for r in range(n_row):
        for c in range(n_col):
            to_r, to_pair, to_side = dest(r, c // 2, c % 2)
            to_c = to_pair * 2 + to_side
            pairs.append((r * n_col + c, to_r % n_row * n_col + to_c % n_col))
    return lax.ppermute(shard, AXES, pairs)


def swap(shard):
    return send(shard, lambda r, pair, side: (r, pair, 1 - side))


def pieces(value):
    high = value.astype(jnp.bfloat16)
    rest = value - high.astype(jnp.float32)
    middle = rest.astype(jnp.bfloat16)
    low = (rest - middle.astype(jnp.float32)).astype(jnp.bfloat16)
    return high, middle, low


def diagonal(slots):
    return lax.broadcasted_iota(jnp.int32, (slots, slots), 0) == lax.broadcasted_iota(jnp.int32, (slots, slots), 1)


def pick(lines, width):
    columns = []
    for line in lines:
        slots = line.shape[1]
        spread = jnp.where(diagonal(slots), jnp.broadcast_to(line, (slots, slots)), 0)
        columns.append(jnp.sum(spread, axis=1, keepdims=True))
    column = jnp.concatenate(columns, axis=0)
    chosen = column == lax.broadcasted_iota(jnp.int32, (column.shape[0], width), 1)
    return chosen.astype(jnp.float32).astype(jnp.bfloat16)


def by_side(action):
    here = lax.axis_index("col") % 2
    for side in range(2):
        pl.when(here == side)(functools.partial(action, side))


def gather(side, block_of, index_ref, refs, out_ref, contract):
    slots = index_ref.shape[2]
    blocks = {}
    for place, (a, b, s) in enumerate(TERMS[side]):
        blocks.setdefault(block_of(a, b, a + b + s - 2 * side), []).append((place, a, b))
    for (which, at), wanted in blocks.items():
        width = out_ref.shape[1]
        chosen = pick([index_ref[(b ^ side) * 2 + a] for _, a, b in wanted], width)
        block = refs[which][at * width : (at + 1) * width, :]
        taken = sum(
            lax.dot_general(chosen, piece, (((1,), (contract,)), ((), ())), preferred_element_type=jnp.float32)
            for piece in pieces(block)
        )
        for n, (place, _, _) in enumerate(wanted):
            out_ref[place * slots : (place + 1) * slots, :] = taken[n * slots : (n + 1) * slots]


def gather_x_kernel(index_ref, own_ref, partner_ref, out_ref):
    @by_side
    def _(side):
        gather(1 - side, lambda a, b, g: (g ^ side, a), index_ref, (own_ref, partner_ref), out_ref, 0)


def gather_z_kernel(index_ref, own_ref, partner_ref, out_ref):
    @by_side
    def _(side):
        gather(1 - side, lambda a, b, g: (b ^ side, g), index_ref, (own_ref, partner_ref), out_ref, 1)


def dots_kernel(x_ref, z_ref, own_ref, other_ref):
    slots = own_ref.shape[2]

    def line(values):
        spread = jnp.where(diagonal(slots), jnp.broadcast_to(values, (slots, slots)), 0.0)
        return jnp.sum(spread, axis=0, keepdims=True)

    @by_side
    def _(side):
        products = [x_ref[n * slots : (n + 1) * slots, :] * z_ref[n * slots : (n + 1) * slots, :] for n in range(len(TERMS[side]))]
        for b in range(2):
            for a in range(2):
                mine = [products[n] for n, term in enumerate(TERMS[side]) if term[:2] == (a, b)]
                if mine:
                    out = line(jnp.sum(sum(mine[1:], mine[0]), axis=1, keepdims=True))
                    if b == side:
                        own_ref[a] = out
                    else:
                        other_ref[0] = out


def finish_kernel(own_ref, other_ref, count_ref, out_ref):
    slots = out_ref.shape[2]
    slot = lax.broadcasted_iota(jnp.int32, (1, slots), 1)
    shared = 1 - lax.axis_index("col") % 2
    for a in range(2):
        value = own_ref[a] + jnp.where(shared == a, other_ref[0], 0.0)
        out_ref[a] = jnp.where(slot < count_ref[a], value, 0.0)


def call(kernel, shapes, *operands):
    return pl.pallas_call(
        kernel,
        out_shape=[jax.ShapeDtypeStruct(shape, jnp.float32) for shape in shapes],
        in_specs=[VMEM] * len(operands),
        out_specs=[VMEM] * len(shapes),
        compiler_params=PARAMS,
    )(*operands)


def body(x_iterate, z_inverse, edge_src, edge_dst, edge_count):
    width = x_iterate.shape[1]
    slots = edge_src.shape[2]
    assert x_iterate.shape[0] == 2 * width
    src_partner = swap(edge_src)
    dst_partner = swap(edge_dst)
    x_partner = swap(x_iterate)
    z_partner = swap(z_inverse)
    src = jnp.concatenate([edge_src, src_partner], axis=0)
    dst = jnp.concatenate([edge_dst, dst_partner], axis=0)
    src = send(src, lambda r, pair, side: (r, pair + r + side, 1 - side))
    dst = send(dst, lambda r, pair, side: (r + pair + side, pair, 1 - side))
    terms = [(len(TERMS[0]) * slots, width)]
    (rows,) = call(gather_x_kernel, terms, src, x_iterate, x_partner)
    rows = send(rows, lambda r, pair, side: (r, pair - r - 1 + side, 1 - side))
    (columns,) = call(gather_z_kernel, terms, dst, z_inverse, z_partner)
    columns = send(columns, lambda r, pair, side: (r - pair - 1 + side, pair, 1 - side))
    own, other = call(dots_kernel, [(2, 1, slots), (1, 1, slots)], rows, columns)
    other = swap(other)
    (out,) = call(finish_kernel, [(2, 1, slots)], own, other, edge_count.reshape(2, 1, 1))
    return out


def solution(mesh):
    return jax.shard_map(
        body,
        mesh=mesh,
        in_specs=(
            P("row", "col"),
            P("row", "col"),
            P("row", "col", None),
            P("row", "col", None),
            P("row", "col"),
        ),
        out_specs=P("row", "col", None),
        check_vma=False,
    )
```

```python
import functools

import jax
import jax.numpy as jnp
from jax import lax
from jax.experimental import pallas as pl
from jax.experimental.pallas import tpu as pltpu
from jax.sharding import PartitionSpec as P


AXES = ("row", "col")
VMEM = pl.BlockSpec(memory_space=pltpu.VMEM)
PARAMS = pltpu.CompilerParams(vmem_limit_bytes=8 * 2**20)

TERMS = tuple(
    tuple((a, b, s) for a in range(2) for b in range(2) for s in range(2) if (a + b + s) // 2 == side)
    for side in range(2)
)


def send(shard, dest):
    n_row, n_col = lax.axis_size("row"), lax.axis_size("col")
    pairs = []
    for r in range(n_row):
        for c in range(n_col):
            to_r, to_pair, to_side = dest(r, c // 2, c % 2)
            to_c = to_pair * 2 + to_side
            pairs.append((r * n_col + c, to_r % n_row * n_col + to_c % n_col))
    return lax.ppermute(shard, AXES, pairs)


def swap(shard):
    return send(shard, lambda r, pair, side: (r, pair, 1 - side))


def pieces(value):
    high = value.astype(jnp.bfloat16)
    rest = value - high.astype(jnp.float32)
    middle = rest.astype(jnp.bfloat16)
    low = (rest - middle.astype(jnp.float32)).astype(jnp.bfloat16)
    return high, middle, low


def diagonal(slots):
    return lax.broadcasted_iota(jnp.int32, (slots, slots), 0) == lax.broadcasted_iota(jnp.int32, (slots, slots), 1)


def eye_kernel(eye_ref):
    eye_ref[...] = diagonal(eye_ref.shape[0]).astype(jnp.float32)


def pick(lines, width, eye):
    columns = []
    for line in lines:
        slots = line.shape[1]
        spread = jnp.where(eye, jnp.broadcast_to(line, (slots, slots)), 0)
        columns.append(jnp.sum(spread, axis=1, keepdims=True))
    column = jnp.concatenate(columns, axis=0)
    chosen = column == lax.broadcasted_iota(jnp.int32, (column.shape[0], width), 1)
    return chosen.astype(jnp.float32).astype(jnp.bfloat16)


def by_side(action):
    here = lax.axis_index("col") % 2
    for side in range(2):
        pl.when(here == side)(functools.partial(action, side))


def gather(side, block_of, index_ref, refs, out_ref, contract, eye):
    slots = index_ref.shape[2]
    blocks = {}
    for place, (a, b, s) in enumerate(TERMS[side]):
        blocks.setdefault(block_of(a, b, a + b + s - 2 * side), []).append((place, a, b))
    for (which, at), wanted in blocks.items():
        width = out_ref.shape[1]
        chosen = pick([index_ref[(b ^ side) * 2 + a] for _, a, b in wanted], width, eye)
        block = refs[which][at * width : (at + 1) * width, :]
        taken = sum(
            lax.dot_general(chosen, piece, (((1,), (contract,)), ((), ())), preferred_element_type=jnp.float32)
            for piece in pieces(block)
        )
        for n, (place, _, _) in enumerate(wanted):
            out_ref[place * slots : (place + 1) * slots, :] = taken[n * slots : (n + 1) * slots]


def gather_x_kernel(index_ref, own_ref, partner_ref, eye_ref, out_ref):
    eye = eye_ref[...] > 0

    @by_side
    def _(side):
        gather(1 - side, lambda a, b, g: (g ^ side, a), index_ref, (own_ref, partner_ref), out_ref, 0, eye)


def gather_z_kernel(index_ref, own_ref, partner_ref, eye_ref, out_ref):
    eye = eye_ref[...] > 0

    @by_side
    def _(side):
        gather(1 - side, lambda a, b, g: (b ^ side, g), index_ref, (own_ref, partner_ref), out_ref, 1, eye)


def dots_kernel(x_ref, z_ref, own_ref, other_ref):
    slots = own_ref.shape[2]

    def line(values):
        spread = jnp.where(diagonal(slots), jnp.broadcast_to(values, (slots, slots)), 0.0)
        return jnp.sum(spread, axis=0, keepdims=True)

    @by_side
    def _(side):
        products = [x_ref[n * slots : (n + 1) * slots, :] * z_ref[n * slots : (n + 1) * slots, :] for n in range(len(TERMS[side]))]
        for b in range(2):
            for a in range(2):
                mine = [products[n] for n, term in enumerate(TERMS[side]) if term[:2] == (a, b)]
                if mine:
                    out = line(jnp.sum(sum(mine[1:], mine[0]), axis=1, keepdims=True))
                    if b == side:
                        own_ref[a] = out
                    else:
                        other_ref[0] = out


def finish_kernel(own_ref, other_ref, count_ref, out_ref):
    slots = out_ref.shape[2]
    slot = lax.broadcasted_iota(jnp.int32, (1, slots), 1)
    shared = 1 - lax.axis_index("col") % 2
    for a in range(2):
        value = own_ref[a] + jnp.where(shared == a, other_ref[0], 0.0)
        out_ref[a] = jnp.where(slot < count_ref[a], value, 0.0)


def call(kernel, shapes, *operands, cost=None):
    return pl.pallas_call(
        kernel,
        out_shape=[jax.ShapeDtypeStruct(shape, jnp.float32) for shape in shapes],
        in_specs=[VMEM] * len(operands),
        out_specs=[VMEM] * len(shapes),
        compiler_params=PARAMS,
        cost_estimate=cost,
    )(*operands)


def body(x_iterate, z_inverse, edge_src, edge_dst, edge_count):
    width = x_iterate.shape[1]
    slots = edge_src.shape[2]
    assert x_iterate.shape[0] == 2 * width
    src_partner = swap(edge_src)
    dst_partner = swap(edge_dst)
    x_partner = swap(x_iterate)
    z_partner = swap(z_inverse)
    (eye,) = call(eye_kernel, [(slots, slots)], cost=pl.CostEstimate(flops=2 * 10**9, bytes_accessed=16384, transcendentals=0))
    src = jnp.concatenate([edge_src, src_partner], axis=0)
    dst = jnp.concatenate([edge_dst, dst_partner], axis=0)
    src = send(src, lambda r, pair, side: (r, pair + r + side, 1 - side))
    dst = send(dst, lambda r, pair, side: (r + pair + side, pair, 1 - side))
    terms = [(len(TERMS[0]) * slots, width)]
    (rows,) = call(gather_x_kernel, terms, src, x_iterate, x_partner, eye)
    rows = send(rows, lambda r, pair, side: (r, pair - r - 1 + side, 1 - side))
    (columns,) = call(gather_z_kernel, terms, dst, z_inverse, z_partner, eye)
    columns = send(columns, lambda r, pair, side: (r - pair - 1 + side, pair, 1 - side))
    own, other = call(dots_kernel, [(2, 1, slots), (1, 1, slots)], rows, columns)
    other = swap(other)
    (out,) = call(finish_kernel, [(2, 1, slots)], own, other, edge_count.reshape(2, 1, 1))
    return out


def solution(mesh):
    return jax.shard_map(
        body,
        mesh=mesh,
        in_specs=(
            P("row", "col"),
            P("row", "col"),
            P("row", "col", None),
            P("row", "col", None),
            P("row", "col"),
        ),
        out_specs=P("row", "col", None),
        check_vma=False,
    )
```

```python
import functools

import jax
import jax.numpy as jnp
from jax import lax
from jax.experimental import pallas as pl
from jax.experimental.pallas import tpu as pltpu
from jax.sharding import PartitionSpec as P


AXES = ("row", "col")
VMEM = pl.BlockSpec(memory_space=pltpu.VMEM)
PARAMS = pltpu.CompilerParams(vmem_limit_bytes=8 * 2**20)


def terms_of(side):
    split = ([], [])
    for a in range(2):
        for s in range(2):
            total = a + side + s
            split[total // 2 != side].append((a, total % 2))
    return split


def send(shard, dest):
    n_row, n_col = lax.axis_size("row"), lax.axis_size("col")
    pairs = []
    for r in range(n_row):
        for c in range(n_col):
            to_r, to_pair, to_side = dest(r, c // 2, c % 2)
            to_c = to_pair * 2 + to_side
            pairs.append((r * n_col + c, to_r % n_row * n_col + to_c % n_col))
    return lax.ppermute(shard, AXES, pairs)


def swap(shard):
    return send(shard, lambda r, pair, side: (r, pair, 1 - side))


def pieces(value):
    high = value.astype(jnp.bfloat16)
    rest = value - high.astype(jnp.float32)
    middle = rest.astype(jnp.bfloat16)
    low = (rest - middle.astype(jnp.float32)).astype(jnp.bfloat16)
    return high, middle, low


def diagonal(slots):
    return lax.broadcasted_iota(jnp.int32, (slots, slots), 0) == lax.broadcasted_iota(jnp.int32, (slots, slots), 1)


def eye_kernel(eye_ref):
    eye_ref[...] = diagonal(eye_ref.shape[0]).astype(jnp.float32)


def pick(lines, width, eye):
    columns = []
    for line in lines:
        slots = line.shape[1]
        spread = jnp.where(eye, jnp.broadcast_to(line, (slots, slots)), 0)
        columns.append(jnp.sum(spread, axis=1, keepdims=True))
    column = jnp.concatenate(columns, axis=0)
    chosen = column == lax.broadcasted_iota(jnp.int32, (column.shape[0], width), 1)
    return chosen.astype(jnp.float32).astype(jnp.bfloat16)


def by_side(action):
    here = lax.axis_index("col") % 2
    for side in range(2):
        pl.when(here == side)(functools.partial(action, side))


def gather_kernel(spare, of_x, index_ref, own_ref, partner_ref, eye_ref, out_ref):
    width = out_ref.shape[1]
    slots = index_ref.shape[2]
    eye = eye_ref[...] > 0

    @by_side
    def _(side):
        blocks = {}
        for place, (a, g) in enumerate(terms_of(1 - side)[spare]):
            blocks.setdefault((g != side, a) if of_x else (True, g), []).append((place, a))
        for (partner, at), wanted in blocks.items():
            chosen = pick([index_ref[a] for _, a in wanted], width, eye)
            block = (partner_ref if partner else own_ref)[at * width : (at + 1) * width, :]
            taken = sum(
                lax.dot_general(
                    chosen, piece, (((1,), (0 if of_x else 1,)), ((), ())), preferred_element_type=jnp.float32
                )
                for piece in pieces(block)
            )
            for n, (place, _) in enumerate(wanted):
                out_ref[place * slots : (place + 1) * slots, :] = taken[n * slots : (n + 1) * slots]


def line(values, eye):
    slots = eye.shape[0]
    spread = jnp.where(eye, jnp.broadcast_to(jnp.sum(values, axis=1, keepdims=True), (slots, slots)), 0.0)
    return jnp.sum(spread, axis=0, keepdims=True)


def finish_kernel(x_main, x_spare, z_main, z_spare, count_ref, eye_ref, out_ref):
    slots = out_ref.shape[2]
    slot = lax.broadcasted_iota(jnp.int32, (1, slots), 1)
    eye = eye_ref[...] > 0

    @by_side
    def _(side):
        for a in range(2):
            products = []
            for terms, x_ref, z_ref in zip(terms_of(side), (x_main, x_spare), (z_main, z_spare)):
                for n, term in enumerate(terms):
                    if term[0] == a:
                        at = slice(n * slots, (n + 1) * slots)
                        products.append(x_ref[at, :] * z_ref[at, :])
            out_ref[a] = jnp.where(slot < count_ref[a], line(sum(products[1:], products[0]), eye), 0.0)


def call(kernel, shapes, *operands, cost=None):
    return pl.pallas_call(
        kernel,
        out_shape=[jax.ShapeDtypeStruct(shape, jnp.float32) for shape in shapes],
        in_specs=[VMEM] * len(operands),
        out_specs=[VMEM] * len(shapes),
        compiler_params=PARAMS,
        cost_estimate=cost,
    )(*operands)


def body(x_iterate, z_inverse, edge_src, edge_dst, edge_count):
    width = x_iterate.shape[1]
    slots = edge_src.shape[2]
    assert x_iterate.shape[0] == 2 * width
    x_partner = swap(x_iterate)
    z_partner = swap(z_inverse)
    (eye,) = call(eye_kernel, [(slots, slots)], cost=pl.CostEstimate(flops=2 * 10**9, bytes_accessed=16384, transcendentals=0))

    def request_x(spare):
        return lambda r, pair, side: (r, pair + r + (side ^ spare), 1 - side)

    def reply_x(spare):
        return lambda r, pair, side: (r, pair - r - (1 - side ^ spare), 1 - side)

    def request_z(spare):
        return lambda r, pair, side: (r + pair + (side ^ spare), pair, 1 - side)

    def reply_z(spare):
        return lambda r, pair, side: (r - pair - (1 - side ^ spare), pair, 1 - side)

    x_got, z_got = [], []
    for spare in range(2):
        shape = [(len(terms_of(0)[spare]) * slots, width)]
        src = send(edge_src, request_x(spare))
        (rows,) = call(functools.partial(gather_kernel, spare, True), shape, src, x_iterate, x_partner, eye)
        x_got.append(send(rows, reply_x(spare)))
        dst = send(edge_dst, request_z(spare))
        (columns,) = call(functools.partial(gather_kernel, spare, False), shape, dst, eye, z_partner, eye)
        z_got.append(send(columns, reply_z(spare)))
    count = edge_count.reshape(2, 1, 1)
    (out,) = call(finish_kernel, [(2, 1, slots)], *x_got, *z_got, count, eye)
    return out


def solution(mesh):
    return jax.shard_map(
        body,
        mesh=mesh,
        in_specs=(
            P("row", "col"),
            P("row", "col"),
            P("row", "col", None),
            P("row", "col", None),
            P("row", "col"),
        ),
        out_specs=P("row", "col", None),
        check_vma=False,
    )
```

```python
import functools

import jax
import jax.numpy as jnp
from jax import lax
from jax.experimental import pallas as pl
from jax.experimental.pallas import tpu as pltpu
from jax.sharding import PartitionSpec as P


AXES = ("row", "col")
VMEM = pl.BlockSpec(memory_space=pltpu.VMEM)
PARAMS = pltpu.CompilerParams(vmem_limit_bytes=8 * 2**20)


def terms_of(side):
    split = ([], [])
    for a in range(2):
        for s in range(2):
            total = a + side + s
            split[total // 2 != side].append((a, total % 2))
    return split


def send(shard, dest):
    n_row, n_col = lax.axis_size("row"), lax.axis_size("col")
    pairs = []
    for r in range(n_row):
        for c in range(n_col):
            to_r, to_pair, to_side = dest(r, c // 2, c % 2)
            to_c = to_pair * 2 + to_side
            pairs.append((r * n_col + c, to_r % n_row * n_col + to_c % n_col))
    return lax.ppermute(shard, AXES, pairs)


def swap(shard):
    return send(shard, lambda r, pair, side: (r, pair, 1 - side))


def pieces(value):
    high = value.astype(jnp.bfloat16)
    rest = value - high.astype(jnp.float32)
    middle = rest.astype(jnp.bfloat16)
    low = (rest - middle.astype(jnp.float32)).astype(jnp.bfloat16)
    return high, middle, low


def diagonal(slots):
    return lax.broadcasted_iota(jnp.int32, (slots, slots), 0) == lax.broadcasted_iota(jnp.int32, (slots, slots), 1)


def eye_kernel(eye_ref):
    eye_ref[...] = diagonal(eye_ref.shape[0]).astype(jnp.float32)


def pick(lines, width, eye):
    columns = []
    for line in lines:
        slots = line.shape[1]
        spread = jnp.where(eye, jnp.broadcast_to(line, (slots, slots)), 0)
        columns.append(jnp.sum(spread, axis=1, keepdims=True))
    column = jnp.concatenate(columns, axis=0)
    chosen = column == lax.broadcasted_iota(jnp.int32, (column.shape[0], width), 1)
    return chosen.astype(jnp.float32).astype(jnp.bfloat16)


def by_side(action):
    here = lax.axis_index("col") % 2
    for side in range(2):
        pl.when(here == side)(functools.partial(action, side))


def gather_kernel(spare, of_x, index_ref, own_ref, partner_ref, eye_ref, out_ref):
    width = out_ref.shape[1]
    slots = index_ref.shape[2]
    eye = eye_ref[...] > 0

    @by_side
    def _(side):
        blocks = {}
        for place, (a, g) in enumerate(terms_of(1 - side)[spare]):
            blocks.setdefault((g != side, a) if of_x else (True, g), []).append((place, a))
        for (partner, at), wanted in blocks.items():
            chosen = pick([index_ref[a] for _, a in wanted], width, eye)
            block = (partner_ref if partner else own_ref)[at * width : (at + 1) * width, :]
            taken = sum(
                lax.dot_general(
                    chosen, piece, (((1,), (0 if of_x else 1,)), ((), ())), preferred_element_type=jnp.float32
                )
                for piece in pieces(block)
            )
            for n, (place, _) in enumerate(wanted):
                out_ref[place * slots : (place + 1) * slots, :] = taken[n * slots : (n + 1) * slots]


def line(values, eye):
    slots = eye.shape[0]
    spread = jnp.where(eye, jnp.broadcast_to(jnp.sum(values, axis=1, keepdims=True), (slots, slots)), 0.0)
    return jnp.sum(spread, axis=0, keepdims=True)


def dots(spare, a, side, x_ref, z_ref, slots):
    products = []
    for n, term in enumerate(terms_of(side)[spare]):
        if term[0] == a:
            at = slice(n * slots, (n + 1) * slots)
            products.append(x_ref[at, :] * z_ref[at, :])
    return sum(products[1:], products[0]) if products else None


def part_kernel(x_main, z_main, eye_ref, out_ref):
    slots = out_ref.shape[2]
    eye = eye_ref[...] > 0

    @by_side
    def _(side):
        for a in range(2):
            out_ref[a] = line(dots(0, a, side, x_main, z_main, slots), eye)


def finish_kernel(part_ref, x_spare, z_spare, count_ref, eye_ref, out_ref):
    slots = out_ref.shape[2]
    slot = lax.broadcasted_iota(jnp.int32, (1, slots), 1)
    eye = eye_ref[...] > 0

    @by_side
    def _(side):
        for a in range(2):
            value = part_ref[a]
            more = dots(1, a, side, x_spare, z_spare, slots)
            if more is not None:
                value = value + line(more, eye)
            out_ref[a] = jnp.where(slot < count_ref[a], value, 0.0)


def call(kernel, shapes, *operands, cost=None):
    return pl.pallas_call(
        kernel,
        out_shape=[jax.ShapeDtypeStruct(shape, jnp.float32) for shape in shapes],
        in_specs=[VMEM] * len(operands),
        out_specs=[VMEM] * len(shapes),
        compiler_params=PARAMS,
        cost_estimate=cost,
    )(*operands)


def body(x_iterate, z_inverse, edge_src, edge_dst, edge_count):
    width = x_iterate.shape[1]
    slots = edge_src.shape[2]
    assert x_iterate.shape[0] == 2 * width
    x_partner = swap(x_iterate)
    z_partner = swap(z_inverse)
    (eye,) = call(eye_kernel, [(slots, slots)], cost=pl.CostEstimate(flops=2 * 10**9, bytes_accessed=16384, transcendentals=0))

    def request_x(spare):
        return lambda r, pair, side: (r, pair + r + (side ^ spare), 1 - side)

    def reply_x(spare):
        return lambda r, pair, side: (r, pair - r - (1 - side ^ spare), 1 - side)

    def request_z(spare):
        return lambda r, pair, side: (r + pair + (side ^ spare), pair, 1 - side)

    def reply_z(spare):
        return lambda r, pair, side: (r - pair - (1 - side ^ spare), pair, 1 - side)

    x_got, z_got = [], []
    for spare in range(2):
        shape = [(len(terms_of(0)[spare]) * slots, width)]
        src = send(edge_src, request_x(spare))
        (rows,) = call(functools.partial(gather_kernel, spare, True), shape, src, x_iterate, x_partner, eye)
        x_got.append(send(rows, reply_x(spare)))
        dst = send(edge_dst, request_z(spare))
        (columns,) = call(functools.partial(gather_kernel, spare, False), shape, dst, eye, z_partner, eye)
        z_got.append(send(columns, reply_z(spare)))
    count = edge_count.reshape(2, 1, 1)
    (part,) = call(part_kernel, [(2, 1, slots)], x_got[0], z_got[0], eye)
    (out,) = call(finish_kernel, [(2, 1, slots)], part, x_got[1], z_got[1], count, eye)
    return out


def solution(mesh):
    return jax.shard_map(
        body,
        mesh=mesh,
        in_specs=(
            P("row", "col"),
            P("row", "col"),
            P("row", "col", None),
            P("row", "col", None),
            P("row", "col"),
        ),
        out_specs=P("row", "col", None),
        check_vma=False,
    )
```

```python
import functools

import jax
import jax.numpy as jnp
from jax import lax
from jax.experimental import pallas as pl
from jax.experimental.pallas import tpu as pltpu
from jax.sharding import PartitionSpec as P


AXES = ("row", "col")
VMEM = pl.BlockSpec(memory_space=pltpu.VMEM)
PARAMS = pltpu.CompilerParams(vmem_limit_bytes=8 * 2**20)


def terms_of(side):
    split = ([], [])
    for a in range(2):
        for s in range(2):
            total = a + side + s
            split[total // 2 != side].append((a, total % 2))
    return split


def send(shard, dest):
    n_row, n_col = lax.axis_size("row"), lax.axis_size("col")
    pairs = []
    for r in range(n_row):
        for c in range(n_col):
            to_r, to_pair, to_side = dest(r, c // 2, c % 2)
            to_c = to_pair * 2 + to_side
            pairs.append((r * n_col + c, to_r % n_row * n_col + to_c % n_col))
    return lax.ppermute(shard, AXES, pairs)


def swap(shard):
    return send(shard, lambda r, pair, side: (r, pair, 1 - side))


def pieces(value):
    high = value.astype(jnp.bfloat16)
    rest = value - high.astype(jnp.float32)
    middle = rest.astype(jnp.bfloat16)
    low = (rest - middle.astype(jnp.float32)).astype(jnp.bfloat16)
    return high, middle, low


def diagonal(slots):
    return lax.broadcasted_iota(jnp.int32, (slots, slots), 0) == lax.broadcasted_iota(jnp.int32, (slots, slots), 1)


def eye_kernel(eye_ref):
    eye_ref[...] = diagonal(eye_ref.shape[0]).astype(jnp.float32)


def pick(lines, width):
    line = jnp.concatenate(lines, axis=1)
    chosen = line == lax.broadcasted_iota(jnp.int32, (width, line.shape[1]), 0)
    return chosen.astype(jnp.float32).astype(jnp.bfloat16)


def by_side(action):
    here = lax.axis_index("col") % 2
    for side in range(2):
        pl.when(here == side)(functools.partial(action, side))


def gather_kernel(spare, of_x, index_ref, own_ref, partner_ref, eye_ref, out_ref):
    width = out_ref.shape[1]
    slots = index_ref.shape[2]

    @by_side
    def _(side):
        blocks = {}
        for place, (a, g) in enumerate(terms_of(1 - side)[spare]):
            blocks.setdefault((g != side, a) if of_x else (True, g), []).append((place, a))
        for (partner, at), wanted in blocks.items():
            chosen = pick([index_ref[a] for _, a in wanted], width)
            block = (partner_ref if partner else own_ref)[at * width : (at + 1) * width, :]
            taken = sum(
                lax.dot_general(
                    chosen, piece, (((0,), (0 if of_x else 1,)), ((), ())), preferred_element_type=jnp.float32
                )
                for piece in pieces(block)
            )
            for n, (place, _) in enumerate(wanted):
                out_ref[place * slots : (place + 1) * slots, :] = taken[n * slots : (n + 1) * slots]


def line(values, eye):
    slots = eye.shape[0]
    spread = jnp.where(eye, jnp.broadcast_to(jnp.sum(values, axis=1, keepdims=True), (slots, slots)), 0.0)
    return jnp.sum(spread, axis=0, keepdims=True)


def dots(spare, a, side, x_ref, z_ref, slots):
    products = []
    for n, term in enumerate(terms_of(side)[spare]):
        if term[0] == a:
            at = slice(n * slots, (n + 1) * slots)
            products.append(x_ref[at, :] * z_ref[at, :])
    return sum(products[1:], products[0]) if products else None


def part_kernel(x_main, z_main, eye_ref, out_ref):
    slots = out_ref.shape[2]
    eye = eye_ref[...] > 0

    @by_side
    def _(side):
        for a in range(2):
            out_ref[a] = line(dots(0, a, side, x_main, z_main, slots), eye)


def finish_kernel(part_ref, x_spare, z_spare, count_ref, eye_ref, out_ref):
    slots = out_ref.shape[2]
    slot = lax.broadcasted_iota(jnp.int32, (1, slots), 1)
    eye = eye_ref[...] > 0

    @by_side
    def _(side):
        for a in range(2):
            value = part_ref[a]
            more = dots(1, a, side, x_spare, z_spare, slots)
            if more is not None:
                value = value + line(more, eye)
            out_ref[a] = jnp.where(slot < count_ref[a], value, 0.0)


def call(kernel, shapes, *operands, cost=None):
    return pl.pallas_call(
        kernel,
        out_shape=[jax.ShapeDtypeStruct(shape, jnp.float32) for shape in shapes],
        in_specs=[VMEM] * len(operands),
        out_specs=[VMEM] * len(shapes),
        compiler_params=PARAMS,
        cost_estimate=cost,
    )(*operands)


def body(x_iterate, z_inverse, edge_src, edge_dst, edge_count):
    width = x_iterate.shape[1]
    slots = edge_src.shape[2]
    assert x_iterate.shape[0] == 2 * width
    x_partner = swap(x_iterate)
    z_partner = swap(z_inverse)
    (eye,) = call(eye_kernel, [(slots, slots)], cost=pl.CostEstimate(flops=2 * 10**9, bytes_accessed=16384, transcendentals=0))

    def request_x(spare):
        return lambda r, pair, side: (r, pair + r + (side ^ spare), 1 - side)

    def reply_x(spare):
        return lambda r, pair, side: (r, pair - r - (1 - side ^ spare), 1 - side)

    def request_z(spare):
        return lambda r, pair, side: (r + pair + (side ^ spare), pair, 1 - side)

    def reply_z(spare):
        return lambda r, pair, side: (r - pair - (1 - side ^ spare), pair, 1 - side)

    x_got, z_got = [], []
    for spare in range(2):
        shape = [(len(terms_of(0)[spare]) * slots, width)]
        src = send(edge_src, request_x(spare))
        (rows,) = call(functools.partial(gather_kernel, spare, True), shape, src, x_iterate, x_partner, eye)
        x_got.append(send(rows, reply_x(spare)))
        dst = send(edge_dst, request_z(spare))
        (columns,) = call(functools.partial(gather_kernel, spare, False), shape, dst, eye, z_partner, eye)
        z_got.append(send(columns, reply_z(spare)))
    count = edge_count.reshape(2, 1, 1)
    (part,) = call(part_kernel, [(2, 1, slots)], x_got[0], z_got[0], eye)
    (out,) = call(finish_kernel, [(2, 1, slots)], part, x_got[1], z_got[1], count, eye)
    return out


def solution(mesh):
    return jax.shard_map(
        body,
        mesh=mesh,
        in_specs=(
            P("row", "col"),
            P("row", "col"),
            P("row", "col", None),
            P("row", "col", None),
            P("row", "col"),
        ),
        out_specs=P("row", "col", None),
        check_vma=False,
    )
```
